768 devices in a mesh: fsdp: 64 (over x, y, core), grp: 12 (over z).
Axes of the slice: x: 4, y: 8, z: 12, core: 2. Of those that a mesh axis runs over, the one named last changes fastest.
Arguments:
- grad_flat: bfloat16 [12, 32768, 256], P('grp', 'fsdp'), may hold values from -6 to 6
- row_block: int32 [12, 32768], P('grp', 'fsdp'), may hold values from 0 to 127, as said below
- row_index: int32 [12, 32768], P('grp', 'fsdp'), may hold values from 0 to 255
- block_home: int32 [12, 128], P('grp'), may hold values from 0 to 127, as said below
- cov_left: float32 [12, 128, 256, 256], P('grp', 'fsdp'), may hold values from -4 to 4
- cov_right: float32 [12, 128, 256, 256], P('grp', 'fsdp'), may hold values from -4 to 4
- basis_left: bfloat16 [12, 128, 256, 256], P('grp', 'fsdp'), may hold values from -0.375 to 0.375
- basis_right: bfloat16 [12, 128, 256, 256], P('grp', 'fsdp'), may hold values from -0.375 to 0.375
- moment_first: bfloat16 [12, 128, 256, 256], P('grp', 'fsdp'), may hold values from -0.59765625 to 0.59765625
- moment_second: bfloat16 [12, 128, 256, 256], P('grp', 'fsdp'), may hold values from 0.0029907227 to 0.29882812
Outputs:
- cov_left_out: float32 [12, 128, 256, 256], P('grp', 'fsdp')
- cov_right_out: float32 [12, 128, 256, 256], P('grp', 'fsdp')
- first_out: bfloat16 [12, 128, 256, 256], P('grp', 'fsdp')
- second_out: bfloat16 [12, 128, 256, 256], P('grp', 'fsdp')
- flat_update: bfloat16 [12, 32768, 256], P('grp', 'fsdp')
The draws below stay inside these ranges and needn't reach their ends.
Inputs may be any that keep to these rules, and one draw needn't show every extreme that they name: `row_block`: in each group every (block, row) pair appears exactly once. Each device's flat rows are intervals of 8 consecutive rows of one block; from one device exactly 8 rows go to the blocks of each fsdp index (owner of a block = block_home // 2). `block_home`: each group's row is a permutation of 0 to 127; state index h lies on fsdp index h // 2.
All inputs are finite; a program needn't handle non-finite values.
Results may differ from the reference program's by a relative error of at most 0.0025.
The reference program's roundings to bfloat16 on the way count: a program that leaves them out, or rounds other values in their place, can miss the bound.
Values may be sent and summed in bfloat16 or wider, within the bound.
A program may use at most 32 MiB of HBM per device.

```python
import math
import jax
import jax.numpy as jnp
from jax import lax

BLOCK = 256
BLK_DEV = 2
ROWS_DEV = 512
NBLK = 128
N_FSDP = 64
N_GRP = 12


def group_layout(key):
    keys = jax.random.split(key, 4)
    pieces = N_FSDP
    piece_rows = ROWS_DEV // pieces
    base_shift = jax.random.permutation(keys[0], N_FSDP).astype(jnp.int32)
    slot_shift = jax.random.permutation(keys[1], N_FSDP).astype(jnp.int32)
    slot_offset = jax.random.permutation(keys[2], pieces).astype(jnp.int32)
    home_perm = jax.random.permutation(keys[3], NBLK).astype(jnp.int32)
    inverse = jnp.zeros((NBLK,), jnp.int32).at[home_perm].set(jnp.arange(NBLK, dtype=jnp.int32))
    device_ids = jnp.arange(N_FSDP, dtype=jnp.int32)[:, None, None]
    slot_ids = jnp.arange(pieces, dtype=jnp.int32)[None, :, None]
    inner_ids = jnp.arange(piece_rows, dtype=jnp.int32)[None, None, :]
    owner_ids = (base_shift[device_ids] + slot_shift[slot_ids]) % N_FSDP
    offsets = piece_rows * slot_offset[slot_ids] + inner_ids
    homes = owner_ids * BLK_DEV + offsets // BLOCK
    rows_in = offsets % BLOCK
    blocks = inverse[homes]
    shape_flat = (N_FSDP * ROWS_DEV,)
    return (jnp.broadcast_to(blocks, (N_FSDP, pieces, piece_rows)).reshape(shape_flat), jnp.broadcast_to(rows_in, (N_FSDP, pieces, piece_rows)).reshape(shape_flat), home_perm)


def full_layout(key):
    group_keys = jax.random.split(jax.random.fold_in(key, 7331), N_GRP)
    return jax.vmap(group_layout)(group_keys)


def draw_row_block(key, part):
    return full_layout(key)[0]


def draw_row_index(key, part):
    return full_layout(key)[1]


def draw_block_home(key, part):
    return full_layout(key)[2]


def block_levels(rng, dims, shards, low, largest):
    level = 1.0
    for axis_at, shards_of in shards:
        steps = jax.random.uniform(jax.random.fold_in(jax.random.fold_in(rng, 6), axis_at), (shards_of,), jnp.float32, low / len(shards), largest / len(shards))
        level = level * jnp.repeat(jnp.exp(steps), dims[axis_at] // shards_of).reshape((-1,) + (1,) * (len(dims) - 1 - axis_at))
    return level


def bell_draw(own_key, dims, width, reach, cuts=(), kind=jnp.bfloat16):
    values = width * jax.random.normal(own_key, dims, jnp.float32)
    if cuts:
        values = values * block_levels(own_key, dims, cuts, -0.22, 0.18)
    return jnp.clip(values, -reach, reach).astype(kind)


def setup_inputs(seed: int = 0) -> dict:
    splits = jax.random.split(jax.random.key(seed), 11)
    return {
        "grad_flat": bell_draw(splits[0], (N_GRP, NBLK * BLOCK, BLOCK), 1.0, 6.0, ((0, 12), (1, 64))),
        "row_block": draw_row_block(jax.random.fold_in(splits[10], 71), 0),
        "row_index": draw_row_index(jax.random.fold_in(splits[10], 71), 0),
        "block_home": draw_block_home(jax.random.fold_in(splits[10], 71), 0),
        "cov_left": bell_draw(splits[4], (N_GRP, NBLK, BLOCK, BLOCK), 0.5, 4.0, ((0, 12), (1, 64)), jnp.float32),
        "cov_right": bell_draw(splits[5], (N_GRP, NBLK, BLOCK, BLOCK), 0.5, 4.0, ((0, 12), (1, 64)), jnp.float32),
        "basis_left": bell_draw(splits[6], (N_GRP, NBLK, BLOCK, BLOCK), BLOCK ** -0.5, 0.375, ((0, 12), (1, 64))),
        "basis_right": bell_draw(splits[7], (N_GRP, NBLK, BLOCK, BLOCK), BLOCK ** -0.5, 0.375, ((0, 12), (1, 64))),
        "moment_first": bell_draw(splits[8], (N_GRP, NBLK, BLOCK, BLOCK), 0.1, 0.59765625, ((0, 12), (1, 64))),
        "moment_second": jnp.clip(jnp.exp(math.log(0.29882812) - 4.6043535 * jax.random.uniform(splits[9], (N_GRP, NBLK, BLOCK, BLOCK), jnp.float32) ** block_levels(splits[9], (N_GRP, NBLK, BLOCK, BLOCK), ((0, 12), (1, 64)), -0.2, 0.2)), 0.0029907227, 0.29882812).astype(jnp.bfloat16),
    }


clip_rms = 0.25
beta_cov = 0.95
beta_first = 0.95
beta_second = 0.95
epsilon = 1e-08

def owner_step(operands, clip_scale):
    grad_block, left_old, right_old, basis_l, basis_r, first_old, second_old = operands
    clipped = (clip_scale * grad_block.astype(jnp.float32)).astype(jnp.bfloat16)
    left_new = beta_cov * left_old + (1.0 - beta_cov) * jnp.dot(clipped, clipped.T, preferred_element_type=jnp.float32)
    right_new = beta_cov * right_old + (1.0 - beta_cov) * jnp.dot(clipped.T, clipped, preferred_element_type=jnp.float32)
    turned = jnp.dot(basis_l.T, clipped, preferred_element_type=jnp.float32).astype(jnp.bfloat16)
    rotated = jnp.dot(turned, basis_r, preferred_element_type=jnp.float32)
    first_new = beta_first * first_old.astype(jnp.float32) + (1.0 - beta_first) * rotated
    second_new = beta_second * second_old.astype(jnp.float32) + (1.0 - beta_second) * rotated * rotated
    normalized = (first_new / (jnp.sqrt(second_new) + epsilon)).astype(jnp.bfloat16)
    back_left = jnp.dot(basis_l, normalized, preferred_element_type=jnp.float32).astype(jnp.bfloat16)
    update = jnp.dot(back_left, basis_r.T, preferred_element_type=jnp.float32).astype(jnp.bfloat16)
    return (left_new, right_new, first_new.astype(jnp.bfloat16), second_new.astype(jnp.bfloat16), update)

def reference(grad_flat, row_block, row_index, block_home, cov_left, cov_right, basis_left, basis_right, moment_first, moment_second):
    home_slot = jnp.take_along_axis(block_home, row_block, axis=1)
    target_row = (home_slot * BLOCK + row_index).astype(jnp.int32)
    group_ids = jnp.broadcast_to(jnp.arange(N_GRP, dtype=jnp.int32)[:, None], target_row.shape)
    stacked = jnp.zeros((N_GRP, NBLK * BLOCK, BLOCK), grad_flat.dtype).at[group_ids, target_row].set(grad_flat)
    grad_wide = grad_flat.astype(jnp.float32)
    sum_squares = jnp.sum(grad_wide * grad_wide)
    entries = N_GRP * NBLK * BLOCK * BLOCK
    root_mean = jnp.sqrt(sum_squares / entries + 1e-06)
    clip_scale = jnp.minimum(1.0, clip_rms / root_mean)

    def flatten(array):
        return array.reshape(N_GRP * NBLK, BLOCK, BLOCK)

    def per_block(operands):
        return owner_step(operands, clip_scale)
    results = lax.map(per_block, (flatten(stacked), flatten(cov_left), flatten(cov_right), flatten(basis_left), flatten(basis_right), flatten(moment_first), flatten(moment_second)))
    shape_out = (N_GRP, NBLK, BLOCK, BLOCK)
    updates = results[4].reshape(N_GRP, NBLK * BLOCK, BLOCK)
    flat_update = updates[group_ids, target_row]
    return (results[0].reshape(shape_out), results[1].reshape(shape_out), results[2].reshape(shape_out), results[3].reshape(shape_out), flat_update)
```

```python
import functools

import jax
import jax.numpy as jnp
from jax import lax
from jax.experimental import pallas as pl
from jax.experimental.pallas import tpu as pltpu
from jax.sharding import PartitionSpec as P

MESH = pl.DeviceIdType.MESH

CLIP_RMS = 0.25
BETA = 0.95
EPS = 1e-08
PIECE = 8
LANES = 128

STAGE = 9


def iota(shape, dim):
    return lax.broadcasted_iota(jnp.int32, shape, dim)


def hot(hits):
    return jnp.where(hits, 1.0, 0.0).astype(jnp.bfloat16)


def dot(a, b, dims=((1,), (0,))):
    return lax.dot_general(a, b, (dims, ((), ())), preferred_element_type=jnp.float32)


def kernel(
    entries,
    n,
    groups,
    grad_hbm,
    row_block_hbm,
    row_index_hbm,
    home_hbm,
    cov_l_hbm,
    cov_r_hbm,
    basis_l_hbm,
    basis_r_hbm,
    first_hbm,
    second_hbm,
    cov_l_out,
    cov_r_out,
    first_out,
    second_out,
    flat_out,
    grad_v,
    row_block_v,
    row_index_v,
    home_v,
    cov_l_v,
    cov_r_v,
    basis_l_v,
    basis_r_v,
    first_v,
    second_v,
    clipped_v,
    send_a,
    recv_a,
    send_b,
    recv_b,
    meta_out,
    meta_in,
    sum_out,
    sum_in,
    to_owner,
    from_owner,
    to_state,
    from_state,
    flat_v,
    in_sem,
    out_sem,
    send_sem,
    recv_sem,
):
    me = lax.axis_index("fsdp")
    mine = lax.axis_index("grp")
    rows, width = grad_v.shape
    blocks = home_v.shape[1]
    per_owner = cov_l_v.shape[0]
    per_block = width // PIECE

    barrier = pltpu.get_barrier_semaphore()

    def peer(k):
        return lax.rem(me + k, n)

    def mate(k):
        return lax.rem(mine + k, groups)

    def greet(k, carry):
        pl.semaphore_signal(barrier, inc=1, device_id=(peer(k), mine), device_id_type=MESH)
        return carry

    def greet_mate(k, carry):
        pl.semaphore_signal(barrier, inc=1, device_id=(me, mate(k)), device_id_type=MESH)
        return carry

    lax.fori_loop(1, n, greet, 0)
    lax.fori_loop(1, groups, greet_mate, 0)

    loads = [
        pltpu.make_async_copy(source, target, in_sem.at[i])
        for i, (source, target) in enumerate(
            [
                (row_block_hbm, row_block_v),
                (home_hbm, home_v),
                (row_index_hbm, row_index_v),
                (grad_hbm.at[0], grad_v),
                (basis_l_hbm.at[0], basis_l_v),
                (basis_r_hbm.at[0], basis_r_v),
                (first_hbm.at[0], first_v),
                (second_hbm.at[0], second_v),
                (cov_l_hbm.at[0], cov_l_v),
                (cov_r_hbm.at[0], cov_r_v),
            ]
        )
    ]
    for load in loads:
        load.start()
    for load in loads[:3]:
        load.wait()

    lookup = hot(iota((blocks, rows), 0) == row_block_v[...])
    homes = jnp.broadcast_to(home_v[...].astype(jnp.float32), (8, blocks)).astype(jnp.bfloat16)
    home = dot(homes, lookup)[0:1].astype(jnp.int32)
    owner = home // per_owner
    piece = (home % per_owner) * per_block + row_index_v[...] // PIECE
    inner = iota((1, rows), 1) % PIECE
    to_owner[...] = hot(iota((rows, rows), 0) == owner * PIECE + inner)
    label = jnp.sum(
        jnp.where(iota((n, rows), 0) == owner, piece.astype(jnp.float32), 0.0), axis=1, keepdims=True
    ) * (1.0 / PIECE)
    meta_out[:, 0, :] = jnp.broadcast_to(label, (n, LANES))

    loads[3].wait()
    grad = grad_v[...]
    wide = grad.astype(jnp.float32)
    total = jnp.sum(jnp.sum(wide * wide, axis=0, keepdims=True), axis=1, keepdims=True)
    meta_out[:, 1, :] = jnp.broadcast_to(total, (n, LANES))
    send_a[...] = dot(to_owner[...], grad).reshape(n, PIECE, width).astype(jnp.bfloat16)

    pl.semaphore_wait(barrier, n - 1 + groups - 1)

    def send_meta(k, carry):
        pltpu.make_async_remote_copy(
            meta_out.at[peer(k)], meta_in.at[me], send_sem.at[0], recv_sem.at[0],
            device_id=(peer(k), mine), device_id_type=MESH,
        ).start()
        return carry

    def send_rows(k, carry):
        pltpu.make_async_remote_copy(
            send_a.at[peer(k)], recv_a.at[me], send_sem.at[1], recv_sem.at[1],
            device_id=(peer(k), mine), device_id_type=MESH,
        ).start()
        return carry

    def send_sum(k, carry):
        pltpu.make_async_remote_copy(
            sum_out, sum_in.at[mine], send_sem.at[2], recv_sem.at[2],
            device_id=(me, mate(k)), device_id_type=MESH,
        ).start()
        return carry

    def send_update(k, carry):
        pltpu.make_async_remote_copy(
            send_b.at[peer(k)], recv_b.at[me], send_sem.at[3], recv_sem.at[3],
            device_id=(peer(k), mine), device_id_type=MESH,
        ).start()
        return carry

    def wait_for(buffer, count, sem):
        part = buffer.at[pl.ds(0, count)]
        pltpu.make_async_copy(part, part, sem).wait()

    lax.fori_loop(1, n, send_meta, 0)
    lax.fori_loop(1, n, send_rows, 0)
    meta_in[me] = meta_out[me]
    recv_a[me] = send_a[me]

    spread = dot(
        jnp.broadcast_to(owner.astype(jnp.float32), (8, rows)).astype(jnp.bfloat16),
        jnp.ones((8, LANES), jnp.bfloat16),
        ((0,), (0,)),
    )
    place = spread.astype(jnp.int32) + iota((rows, LANES), 0) % PIECE
    for c in range(rows // LANES):
        from_owner[:, c * LANES : (c + 1) * LANES] = hot(iota((rows, LANES), 1) + c * LANES == place)

    wait_for(meta_in, n - 1, recv_sem.at[0])
    sum_out[...] = jnp.sum(meta_in[:, 1, :], axis=0, keepdims=True)
    lax.fori_loop(1, groups, send_sum, 0)
    sum_in[mine] = sum_out[...]

    came = meta_in[:, 0, :]
    came_column = jnp.broadcast_to(meta_in[:, 0:1, :], (n, PIECE, LANES)).reshape(rows, LANES)
    place = came_column.astype(jnp.int32) * PIECE + iota((rows, LANES), 0) % PIECE
    for c in range(rows // LANES):
        to_state_c = hot(iota((rows, LANES), 1) + c * LANES == place)
        from_state[:, c * LANES : (c + 1) * LANES] = to_state_c
    came_row = dot(
        came.astype(jnp.bfloat16), hot(iota((n, rows), 0) == iota((n, rows), 1) // PIECE), ((0,), (0,))
    )[0:1].astype(jnp.int32)
    to_state[...] = hot(iota((rows, rows), 0) == came_row * PIECE + inner)

    for load in loads[4:]:
        load.wait()
    wait_for(recv_a, n - 1, recv_sem.at[1])
    arrived = recv_a[...].astype(jnp.float32).reshape(rows, width).astype(jnp.bfloat16)
    stacked = dot(to_state[...], arrived)

    wait_for(sum_in, groups - 1, recv_sem.at[2])
    sum_squares = jnp.sum(sum_in[:, 0, :], axis=0, keepdims=True)
    scale = jnp.minimum(1.0, CLIP_RMS / jnp.sqrt(sum_squares / entries + 1e-06))[:, 0:1]
    clipped = (scale * stacked).astype(jnp.bfloat16)
    clipped_v[...] = clipped.reshape(per_owner, width, width)

    updates = []
    for b in range(per_owner):
        basis_l = basis_l_v[b]
        basis_r = basis_r_v[b]
        block = clipped[b * width : (b + 1) * width]
        turned = dot(basis_l, block, ((0,), (0,))).astype(jnp.bfloat16)
        rotated = dot(turned, basis_r)
        m = BETA * first_v[b].astype(jnp.float32) + (1.0 - BETA) * rotated
        v = BETA * second_v[b].astype(jnp.float32) + (1.0 - BETA) * rotated * rotated
        first_v[b] = m.astype(jnp.bfloat16)
        second_v[b] = v.astype(jnp.bfloat16)
        normalized = (m / (jnp.sqrt(v) + EPS)).astype(jnp.bfloat16)
        back = dot(basis_l, normalized).astype(jnp.bfloat16)
        updates.append(dot(back, basis_r, ((1,), (1,))).astype(jnp.bfloat16))
    update = jnp.concatenate(updates, axis=0)
    send_b[...] = dot(from_state[...], update).reshape(n, PIECE, width).astype(jnp.bfloat16)
    lax.fori_loop(1, n, send_update, 0)
    recv_b[me] = send_b[me]

    stores = [
        pltpu.make_async_copy(source, target, out_sem.at[i])
        for i, (source, target) in enumerate(
            [
                (first_v, first_out.at[0]),
                (second_v, second_out.at[0]),
                (cov_l_v, cov_l_out.at[0]),
                (cov_r_v, cov_r_out.at[0]),
                (flat_v, flat_out.at[0]),
            ]
        )
    ]
    stores[0].start()
    stores[1].start()
    for b in range(per_owner):
        block = clipped_v[b]
        cov_l_v[b] = BETA * cov_l_v[b] + (1.0 - BETA) * dot(block, block, ((1,), (1,)))
    stores[2].start()
    for b in range(per_owner):
        block = clipped_v[b]
        cov_r_v[b] = BETA * cov_r_v[b] + (1.0 - BETA) * dot(block, block, ((0,), (0,)))
    stores[3].start()

    wait_for(recv_b, n - 1, recv_sem.at[3])
    returned = recv_b[...].astype(jnp.float32).reshape(rows, width).astype(jnp.bfloat16)
    flat_v[...] = dot(from_owner[...], returned).astype(jnp.bfloat16)
    stores[4].start()

    wait_for(meta_out, n - 1, send_sem.at[0])
    wait_for(send_a, n - 1, send_sem.at[1])
    wait_for(sum_in, groups - 1, send_sem.at[2])
    wait_for(send_b, n - 1, send_sem.at[3])
    for store in stores:
        store.wait()


def solution(mesh):
    n = mesh.shape["fsdp"]
    groups = mesh.shape["grp"]

    def shard(grad, row_block, row_index, home, cov_l, cov_r, basis_l, basis_r, first, second):
        rows, width = grad.shape[1:]
        per_owner = cov_l.shape[1]
        block = (per_owner, width, width)
        f32, bf16, i32 = jnp.float32, jnp.bfloat16, jnp.int32
        vmem = pltpu.VMEM
        anywhere = pl.BlockSpec(memory_space=pl.ANY)
        entries = float(n * groups * rows * width)
        return pl.pallas_call(
            functools.partial(kernel, entries, n, groups),
            out_shape=(
                jax.ShapeDtypeStruct(cov_l.shape, f32),
                jax.ShapeDtypeStruct(cov_r.shape, f32),
                jax.ShapeDtypeStruct(first.shape, bf16),
                jax.ShapeDtypeStruct(second.shape, bf16),
                jax.ShapeDtypeStruct(grad.shape, bf16),
            ),
            in_specs=[anywhere] * 10,
            out_specs=(anywhere,) * 5,
            scratch_shapes=[
                vmem((rows, width), bf16),
                vmem(row_block.shape, i32),
                vmem(row_index.shape, i32),
                vmem(home.shape, i32),
                vmem(block, f32),
                vmem(block, f32),
                vmem(block, bf16),
                vmem(block, bf16),
                vmem(block, bf16),
                vmem(block, bf16),
                vmem(block, bf16),
                vmem((n, PIECE, width), bf16),
                vmem((n, PIECE, width), bf16),
                vmem((n, PIECE, width), bf16),
                vmem((n, PIECE, width), bf16),
                vmem((n, 2, LANES), f32),
                vmem((n, 2, LANES), f32),
                vmem((1, LANES), f32),
                vmem((groups, 1, LANES), f32),
                vmem((rows, rows), bf16),
                vmem((rows, rows), bf16),
                vmem((rows, rows), bf16),
                vmem((rows, rows), bf16),
                vmem((rows, width), bf16),
                pltpu.SemaphoreType.DMA((10,)),
                pltpu.SemaphoreType.DMA((5,)),
                pltpu.SemaphoreType.DMA((4,)),
                pltpu.SemaphoreType.DMA((4,)),
            ],
            compiler_params=pltpu.CompilerParams(collective_id=0, has_side_effects=True),
            name="soap_step",
        )(grad, row_block, row_index, home, cov_l, cov_r, basis_l, basis_r, first, second)

    flat = P("grp", "fsdp", None)
    index = P("grp", "fsdp")
    state = P("grp", "fsdp", None, None)
    return jax.shard_map(
        shard,
        mesh=mesh,
        in_specs=(flat, index, index, P("grp", None)) + (state,) * 6,
        out_specs=(state,) * 4 + (flat,),
        check_vma=False,
    )
```

```python
import functools

import jax
import jax.numpy as jnp
from jax import lax
from jax.experimental import pallas as pl
from jax.experimental.pallas import tpu as pltpu
from jax.sharding import PartitionSpec as P

MESH = pl.DeviceIdType.MESH

CLIP_RMS = 0.25
BETA = 0.95
EPS = 1e-08
PIECE = 8
LANES = 128


def iota(shape, dim):
    return lax.broadcasted_iota(jnp.int32, shape, dim)


def hot(hits):
    return jnp.where(hits, 1.0, 0.0).astype(jnp.bfloat16)


def dot(a, b, dims=((1,), (0,))):
    return lax.dot_general(a, b, (dims, ((), ())), preferred_element_type=jnp.float32)


def steps(sizes):
    nx, ny, nc = sizes
    near_y = sorted(range(ny), key=lambda d: -min(d, ny - d))
    near_x = sorted(range(nx), key=lambda d: -min(d, nx - d))
    return [(dx, dy, dc) for dy in near_y for dx in near_x for dc in range(nc) if dx or dy or dc]


def kernel(
    entries,
    sizes,
    groups,
    grad_hbm,
    row_block_hbm,
    row_index_hbm,
    home_hbm,
    cov_l_hbm,
    cov_r_hbm,
    basis_l_hbm,
    basis_r_hbm,
    first_hbm,
    second_hbm,
    cov_l_out,
    cov_r_out,
    first_out,
    second_out,
    flat_out,
    grad_v,
    row_block_v,
    row_index_v,
    home_v,
    cov_l_v,
    cov_r_v,
    basis_l_v,
    basis_r_v,
    basis_l_t,
    first_v,
    second_v,
    stacked_v,
    clipped_v,
    send_a,
    recv_a,
    send_b,
    recv_b,
    meta_out,
    meta_in,
    part_out,
    part_in,
    sum_out,
    sum_in,
    all_out,
    all_in,
    to_owner,
    from_owner,
    to_state,
    from_state,
    in_sem,
    send_sem,
    recv_sem,
):
    me = lax.axis_index("fsdp")
    mine = lax.axis_index("grp")
    nx, ny, nc = sizes
    n = nx * ny * nc
    rows, width = grad_v.shape
    blocks = home_v.shape[1]
    per_owner = cov_l_v.shape[0]
    per_block = width // PIECE
    my_x, my_y, my_c = me // (ny * nc), lax.rem(me // nc, ny), lax.rem(me, nc)

    def peer(step):
        dx, dy, dc = step
        x, y, c = lax.rem(my_x + dx, nx), lax.rem(my_y + dy, ny), lax.rem(my_c + dc, nc)
        return (x * ny + y) * nc + c

    loads = [
        pltpu.make_async_copy(source, target, in_sem.at[i])
        for i, (source, target) in enumerate(
            [
                (grad_hbm.at[0], grad_v),
                (row_block_hbm, row_block_v),
                (home_hbm, home_v),
                (row_index_hbm, row_index_v),
                (basis_l_hbm.at[0], basis_l_v),
                (basis_r_hbm.at[0], basis_r_v),
                (first_hbm.at[0], first_v),
                (second_hbm.at[0], second_v),
                (cov_l_hbm.at[0], cov_l_v),
                (cov_r_hbm.at[0], cov_r_v),
            ]
        )
    ]
    for load in loads:
        load.start()

    barrier = pltpu.get_barrier_semaphore()
    for step in steps(sizes):
        pl.semaphore_signal(barrier, inc=1, device_id=(peer(step), mine), device_id_type=MESH)

    @pl.when(mine == 0)
    def _():
        def greet(g, carry):
            pl.semaphore_signal(barrier, inc=1, device_id=(me, g), device_id_type=MESH)
            return carry

        lax.fori_loop(1, groups, greet, 0)

    def send(source, target, k, to):
        pltpu.make_async_remote_copy(
            source, target, send_sem.at[k], recv_sem.at[k], device_id=to, device_id_type=MESH
        ).start()

    def to_peers(source, target, k):
        for step in steps(sizes):
            to = peer(step)
            send(source.at[to], target.at[me], k, (to, mine))

    def wait_for(buffer, count, sem):
        part = buffer.at[pl.ds(0, count)]
        pltpu.make_async_copy(part, part, sem).wait()

    loads[0].wait()
    wide = grad_v[...].astype(jnp.float32)
    total = jnp.sum(jnp.sum(wide * wide, axis=0, keepdims=True), axis=1, keepdims=True)
    part_out[...] = jnp.broadcast_to(total, (1, LANES))

    @pl.when(mine == 0)
    def _():
        part_in[0] = part_out[...]
        pl.semaphore_wait(barrier, n - 1)

    @pl.when(mine != 0)
    def _():
        pl.semaphore_wait(barrier, n)
        send(part_out, part_in.at[mine], 0, (me, 0))

    for load in loads[1:4]:
        load.wait()
    lookup = hot(iota((blocks, rows), 0) == row_block_v[...])
    homes = jnp.broadcast_to(home_v[...].astype(jnp.float32), (8, blocks)).astype(jnp.bfloat16)
    home = dot(homes, lookup)[0:1].astype(jnp.int32)
    owner = home // per_owner
    piece = (home % per_owner) * per_block + row_index_v[...] // PIECE
    inner = iota((1, rows), 1) % PIECE
    label = jnp.sum(
        jnp.where(iota((n, rows), 0) == owner, piece.astype(jnp.float32), 0.0), axis=1, keepdims=True
    ) * (1.0 / PIECE)
    meta_out[:, 0, :] = jnp.broadcast_to(label, (n, LANES))
    to_owner[...] = hot(iota((rows, rows), 0) == owner * PIECE + inner)
    send_a[...] = dot(to_owner[...], grad_v[...]).reshape(n, PIECE, width).astype(jnp.bfloat16)

    to_peers(meta_out, meta_in, 1)
    to_peers(send_a, recv_a, 2)
    meta_in[me] = meta_out[me]
    recv_a[me] = send_a[me]

    spread = dot(
        jnp.broadcast_to(owner.astype(jnp.float32), (8, rows)).astype(jnp.bfloat16),
        jnp.ones((8, LANES), jnp.bfloat16),
        ((0,), (0,)),
    )
    place = spread.astype(jnp.int32) + iota((rows, LANES), 0) % PIECE
    for c in range(rows // LANES):
        from_owner[:, c * LANES : (c + 1) * LANES] = hot(iota((rows, LANES), 1) + c * LANES == place)
    for load in loads[4:]:
        load.wait()
    for b in range(per_owner):
        basis_l_t[b] = basis_l_v[b].T

    wait_for(meta_in, n - 1, recv_sem.at[1])
    came_column = jnp.broadcast_to(meta_in[...], (n, PIECE, LANES)).reshape(rows, LANES)
    place = came_column.astype(jnp.int32) * PIECE + iota((rows, LANES), 0) % PIECE
    for c in range(rows // LANES):
        from_state[:, c * LANES : (c + 1) * LANES] = hot(iota((rows, LANES), 1) + c * LANES == place)
    came_row = dot(
        meta_in[:, 0, :].astype(jnp.bfloat16),
        hot(iota((n, rows), 0) == iota((n, rows), 1) // PIECE),
        ((0,), (0,)),
    )[0:1].astype(jnp.int32)
    to_state[...] = hot(iota((rows, rows), 0) == came_row * PIECE + inner)

    @pl.when(mine == 0)
    def _():
        wait_for(part_in, groups - 1, recv_sem.at[0])
        sum_out[...] = jnp.sum(part_in[:, 0, :], axis=0, keepdims=True)
        for step in steps(sizes):
            to = peer(step)
            send(sum_out, sum_in.at[me], 3, (to, mine))
        sum_in[me] = sum_out[...]

    wait_for(recv_a, n - 1, recv_sem.at[2])
    arrived = recv_a[...].astype(jnp.float32).reshape(rows, width).astype(jnp.bfloat16)
    stacked_v[...] = dot(to_state[...], arrived)

    @pl.when(mine == 0)
    def _():
        wait_for(sum_in, n - 1, recv_sem.at[3])
        all_out[...] = jnp.sum(sum_in[:, 0, :], axis=0, keepdims=True)

        def tell(g, carry):
            send(all_out, all_in, 4, (me, g))
            return carry

        lax.fori_loop(1, groups, tell, 0)
        all_in[...] = all_out[...]

    @pl.when(mine != 0)
    def _():
        pltpu.make_async_copy(all_in, all_in, recv_sem.at[4]).wait()

    scale = jnp.minimum(1.0, CLIP_RMS / jnp.sqrt(all_in[...] / entries + 1e-06))[:, 0:1]

    updates = []
    for b in range(per_owner):
        basis_l = basis_l_v[b]
        basis_r = basis_r_v[b]
        block = (scale * stacked_v[b * width : (b + 1) * width]).astype(jnp.bfloat16)
        clipped_v[b] = block
        turned = dot(basis_l_t[b], block).astype(jnp.bfloat16)
        rotated = dot(turned, basis_r)
        m = BETA * first_v[b].astype(jnp.float32) + (1.0 - BETA) * rotated
        v = BETA * second_v[b].astype(jnp.float32) + (1.0 - BETA) * rotated * rotated
        first_out[b] = m.astype(jnp.bfloat16)
        second_out[b] = v.astype(jnp.bfloat16)
        normalized = (m / (jnp.sqrt(v) + EPS)).astype(jnp.bfloat16)
        back = dot(basis_l, normalized).astype(jnp.bfloat16)
        updates.append(dot(back, basis_r, ((1,), (1,))).astype(jnp.bfloat16))
    update = jnp.concatenate(updates, axis=0)
    send_b[...] = dot(from_state[...], update).reshape(n, PIECE, width).astype(jnp.bfloat16)
    to_peers(send_b, recv_b, 5)
    recv_b[me] = send_b[me]

    for b in range(per_owner):
        block = clipped_v[b]
        cov_l_out[b] = BETA * cov_l_v[b] + (1.0 - BETA) * dot(block, block, ((1,), (1,)))
        cov_r_out[b] = BETA * cov_r_v[b] + (1.0 - BETA) * dot(block, block, ((0,), (0,)))

    wait_for(meta_out, n - 1, send_sem.at[1])
    wait_for(send_a, n - 1, send_sem.at[2])

    @pl.when(mine == 0)
    def _():
        wait_for(sum_in, n - 1, send_sem.at[3])
        wait_for(part_in, groups - 1, send_sem.at[4])

    @pl.when(mine != 0)
    def _():
        pltpu.make_async_copy(part_out, part_out, send_sem.at[0]).wait()

    wait_for(send_b, n - 1, send_sem.at[5])
    wait_for(recv_b, n - 1, recv_sem.at[5])
    returned = recv_b[...].astype(jnp.float32).reshape(rows, width).astype(jnp.bfloat16)
    flat_out[...] = dot(from_owner[...], returned).astype(jnp.bfloat16)


def keep(*refs):
    half = (len(refs) - 1) // 2
    sources, targets, sem = refs[:half], refs[half : 2 * half], refs[-1]
    stores = [
        pltpu.make_async_copy(source, target.at[0], sem.at[i])
        for i, (source, target) in enumerate(zip(sources, targets))
    ]
    for store in stores:
        store.start()
    for store in stores:
        store.wait()


def solution(mesh):
    n = mesh.shape["fsdp"]
    groups = mesh.shape["grp"]
    sizes = (4, n // 8, 2)

    def shard(grad, row_block, row_index, home, cov_l, cov_r, basis_l, basis_r, first, second):
        rows, width = grad.shape[1:]
        per_owner = cov_l.shape[1]
        block = (per_owner, width, width)
        f32, bf16, i32 = jnp.float32, jnp.bfloat16, jnp.int32
        vmem = pltpu.VMEM
        anywhere = pl.BlockSpec(memory_space=pl.ANY)
        here = pl.BlockSpec(memory_space=pltpu.VMEM)
        entries = float(n * groups * rows * width)
        results = pl.pallas_call(
            functools.partial(kernel, entries, sizes, groups),
            out_shape=(
                jax.ShapeDtypeStruct(block, f32),
                jax.ShapeDtypeStruct(block, f32),
                jax.ShapeDtypeStruct(block, bf16),
                jax.ShapeDtypeStruct(block, bf16),
                jax.ShapeDtypeStruct((rows, width), bf16),
            ),
            in_specs=[pl.BlockSpec(memory_space=pltpu.HBM)] * 10,
            out_specs=(here,) * 5,
            scratch_shapes=[
                vmem((rows, width), bf16),
                vmem(row_block.shape, i32),
                vmem(row_index.shape, i32),
                vmem(home.shape, i32),
                vmem(block, f32),
                vmem(block, f32),
                vmem(block, bf16),
                vmem(block, bf16),
                vmem(block, bf16),
                vmem(block, bf16),
                vmem(block, bf16),
                vmem((rows, width), f32),
                vmem(block, bf16),
                vmem((n, PIECE, width), bf16),
                vmem((n, PIECE, width), bf16),
                vmem((n, PIECE, width), bf16),
                vmem((n, PIECE, width), bf16),
                vmem((n, 1, LANES), f32),
                vmem((n, 1, LANES), f32),
                vmem((1, LANES), f32),
                vmem((groups, 1, LANES), f32),
                vmem((1, LANES), f32),
                vmem((n, 1, LANES), f32),
                vmem((1, LANES), f32),
                vmem((1, LANES), f32),
                vmem((rows, rows), bf16),
                vmem((rows, rows), bf16),
                vmem((rows, rows), bf16),
                vmem((rows, rows), bf16),
                pltpu.SemaphoreType.DMA((10,)),
                pltpu.SemaphoreType.DMA((6,)),
                pltpu.SemaphoreType.DMA((6,)),
            ],
            compiler_params=pltpu.CompilerParams(
                collective_id=0, has_side_effects=True, vmem_limit_bytes=24 * 1024 * 1024
            ),
            name="soap_step",
        )(
            *(
                pltpu.with_memory_space_constraint(x, pltpu.HBM)
                for x in (grad, row_block, row_index, home, cov_l, cov_r, basis_l, basis_r, first, second)
            )
        )
        return pl.pallas_call(
            keep,
            out_shape=tuple(jax.ShapeDtypeStruct((1,) + r.shape, r.dtype) for r in results),
            in_specs=[here] * 5,
            out_specs=(anywhere,) * 5,
            scratch_shapes=[pltpu.SemaphoreType.DMA((5,))],
            compiler_params=pltpu.CompilerParams(vmem_limit_bytes=8 * 1024 * 1024),
            name="keep",
        )(*results)

    flat = P("grp", "fsdp", None)
    index = P("grp", "fsdp")
    state = P("grp", "fsdp", None, None)
    return jax.shard_map(
        shard,
        mesh=mesh,
        in_specs=(flat, index, index, P("grp", None)) + (state,) * 6,
        out_specs=(state,) * 4 + (flat,),
        check_vma=False,
    )
```

```python
import functools

import jax
import jax.numpy as jnp
from jax import lax
from jax.experimental import pallas as pl
from jax.experimental.pallas import tpu as pltpu
from jax.sharding import PartitionSpec as P

MESH = pl.DeviceIdType.MESH

CLIP_RMS = 0.25
BETA = 0.95
EPS = 1e-08
PIECE = 8
LANES = 128


def iota(shape, dim):
    return lax.broadcasted_iota(jnp.int32, shape, dim)


def hot(hits):
    return jnp.where(hits, 1.0, 0.0).astype(jnp.bfloat16)


def dot(a, b, dims=((1,), (0,))):
    return lax.dot_general(a, b, (dims, ((), ())), preferred_element_type=jnp.float32)


def steps(sizes):
    nx, ny, nc = sizes
    near_y = sorted(range(ny), key=lambda d: -min(d, ny - d))
    near_x = sorted(range(nx), key=lambda d: -min(d, nx - d))
    return [(dx, dy, dc) for dy in near_y for dx in near_x for dc in range(nc) if dx or dy or dc]


def kernel(
    entries,
    sizes,
    groups,
    grad_hbm,
    row_block_hbm,
    row_index_hbm,
    home_hbm,
    cov_l_hbm,
    cov_r_hbm,
    basis_l_hbm,
    basis_r_hbm,
    first_hbm,
    second_hbm,
    cov_l_out,
    cov_r_out,
    first_out,
    second_out,
    flat_out,
    grad_v,
    row_block_v,
    row_index_v,
    home_v,
    cov_l_v,
    cov_r_v,
    basis_l_v,
    basis_r_v,
    basis_l_t,
    first_v,
    second_v,
    stacked_v,
    clipped_v,
    send_a,
    recv_a,
    send_b,
    recv_b,
    meta_out,
    meta_in,
    part_out,
    part_in,
    sum_out,
    sum_in,
    all_out,
    all_in,
    to_owner,
    from_owner,
    to_state,
    from_state,
    in_sem,
    send_sem,
    recv_sem,
    up_sem,
    down_sem,
):
    me = lax.axis_index("fsdp")
    mine = lax.axis_index("grp")
    nx, ny, nc = sizes
    n = nx * ny * nc
    rows, width = grad_v.shape
    blocks = home_v.shape[1]
    per_owner = cov_l_v.shape[0]
    per_block = width // PIECE
    my_x, my_y, my_c = me // (ny * nc), lax.rem(me // nc, ny), lax.rem(me, nc)

    def peer(step):
        dx, dy, dc = step
        x, y, c = lax.rem(my_x + dx, nx), lax.rem(my_y + dy, ny), lax.rem(my_c + dc, nc)
        return (x * ny + y) * nc + c

    loads = [
        pltpu.make_async_copy(source, target, in_sem.at[i])
        for i, (source, target) in enumerate(
            [
                (grad_hbm.at[0], grad_v),
                (row_block_hbm, row_block_v),
                (home_hbm, home_v),
                (row_index_hbm, row_index_v),
                (basis_l_hbm.at[0], basis_l_v),
                (basis_r_hbm.at[0], basis_r_v),
                (first_hbm.at[0], first_v),
                (second_hbm.at[0], second_v),
                (cov_l_hbm.at[0], cov_l_v),
                (cov_r_hbm.at[0], cov_r_v),
            ]
        )
    ]
    for load in loads:
        load.start()

    barrier = pltpu.get_barrier_semaphore()
    row = [(dx, 0, dc) for dx in range(nx) for dc in range(nc) if dx or dc]
    above, below = peer((0, 1, 0)), peer((0, ny - 1, 0))
    for to in [above, below] + [peer(step) for step in row]:
        pl.semaphore_signal(barrier, inc=1, device_id=(to, mine), device_id_type=MESH)

    @pl.when(mine == 0)
    def _():
        def greet(g, carry):
            pl.semaphore_signal(barrier, inc=1, device_id=(me, g), device_id_type=MESH)
            return carry

        lax.fori_loop(1, groups, greet, 0)

    def send(source, target, k, to):
        pltpu.make_async_remote_copy(
            source, target, send_sem.at[k], recv_sem.at[k], device_id=to, device_id_type=MESH
        ).start()

    def to_peers(source, target, k):
        for step in steps(sizes):
            to = peer(step)
            send(source.at[to], target.at[me], k, (to, mine))

    def wait_for(buffer, count, sem):
        part = buffer.at[pl.ds(0, count)]
        pltpu.make_async_copy(part, part, sem).wait()

    loads[0].wait()
    wide = grad_v[...].astype(jnp.float32)
    total = jnp.sum(jnp.sum(wide * wide, axis=0, keepdims=True), axis=1, keepdims=True)
    part_out[...] = jnp.broadcast_to(total, (1, LANES))

    @pl.when(mine == 0)
    def _():
        part_in[0] = part_out[...]
        pl.semaphore_wait(barrier, len(row) + 2)

    @pl.when(mine != 0)
    def _():
        pl.semaphore_wait(barrier, len(row) + 3)
        send(part_out, part_in.at[mine], 0, (me, 0))

    def pass_up():
        pl.semaphore_signal(up_sem, inc=1, device_id=(above, mine), device_id_type=MESH)

    def pass_down():
        pl.semaphore_signal(down_sem, inc=1, device_id=(below, mine), device_id_type=MESH)

    pass_up()
    pass_down()

    for load in loads[1:4]:
        load.wait()
    lookup = hot(iota((blocks, rows), 0) == row_block_v[...])
    homes = jnp.broadcast_to(home_v[...].astype(jnp.float32), (8, blocks)).astype(jnp.bfloat16)
    home = dot(homes, lookup)[0:1].astype(jnp.int32)
    owner = home // per_owner
    piece = (home % per_owner) * per_block + row_index_v[...] // PIECE
    inner = iota((1, rows), 1) % PIECE
    label = jnp.sum(
        jnp.where(iota((n, rows), 0) == owner, piece.astype(jnp.float32), 0.0), axis=1, keepdims=True
    ) * (1.0 / PIECE)
    meta_out[:, 0, :] = jnp.broadcast_to(label, (n, LANES))
    to_owner[...] = hot(iota((rows, rows), 0) == owner * PIECE + inner)
    send_a[...] = dot(to_owner[...], grad_v[...]).reshape(n, PIECE, width).astype(jnp.bfloat16)

    ups, downs = ny // 2, ny - 1 - ny // 2
    for k in range(1, ups + 1):
        pl.semaphore_wait(up_sem, 1)
        if k < ups:
            pass_up()
        if k <= downs:
            pl.semaphore_wait(down_sem, 1)
            if k < downs:
                pass_down()

    to_peers(meta_out, meta_in, 1)
    to_peers(send_a, recv_a, 2)
    meta_in[me] = meta_out[me]
    recv_a[me] = send_a[me]

    spread = dot(
        jnp.broadcast_to(owner.astype(jnp.float32), (8, rows)).astype(jnp.bfloat16),
        jnp.ones((8, LANES), jnp.bfloat16),
        ((0,), (0,)),
    )
    place = spread.astype(jnp.int32) + iota((rows, LANES), 0) % PIECE
    for c in range(rows // LANES):
        from_owner[:, c * LANES : (c + 1) * LANES] = hot(iota((rows, LANES), 1) + c * LANES == place)
    for load in loads[4:]:
        load.wait()
    for b in range(per_owner):
        basis_l_t[b] = basis_l_v[b].T

    wait_for(meta_in, n - 1, recv_sem.at[1])
    came_column = jnp.broadcast_to(meta_in[...], (n, PIECE, LANES)).reshape(rows, LANES)
    place = came_column.astype(jnp.int32) * PIECE + iota((rows, LANES), 0) % PIECE
    for c in range(rows // LANES):
        from_state[:, c * LANES : (c + 1) * LANES] = hot(iota((rows, LANES), 1) + c * LANES == place)
    came_row = dot(
        meta_in[:, 0, :].astype(jnp.bfloat16),
        hot(iota((n, rows), 0) == iota((n, rows), 1) // PIECE),
        ((0,), (0,)),
    )[0:1].astype(jnp.int32)
    to_state[...] = hot(iota((rows, rows), 0) == came_row * PIECE + inner)

    @pl.when(mine == 0)
    def _():
        wait_for(part_in, groups - 1, recv_sem.at[0])
        sum_out[...] = jnp.sum(part_in[:, 0, :], axis=0, keepdims=True)
        for step in steps(sizes):
            to = peer(step)
            send(sum_out, sum_in.at[me], 3, (to, mine))
        sum_in[me] = sum_out[...]

    wait_for(recv_a, n - 1, recv_sem.at[2])
    arrived = recv_a[...].astype(jnp.float32).reshape(rows, width).astype(jnp.bfloat16)
    stacked_v[...] = dot(to_state[...], arrived)

    @pl.when(mine == 0)
    def _():
        wait_for(sum_in, n - 1, recv_sem.at[3])
        all_out[...] = jnp.sum(sum_in[:, 0, :], axis=0, keepdims=True)

        def tell(g, carry):
            send(all_out, all_in, 4, (me, g))
            return carry

        lax.fori_loop(1, groups, tell, 0)
        all_in[...] = all_out[...]

    @pl.when(mine != 0)
    def _():
        pltpu.make_async_copy(all_in, all_in, recv_sem.at[4]).wait()

    scale = jnp.minimum(1.0, CLIP_RMS / jnp.sqrt(all_in[...] / entries + 1e-06))
    scale = jnp.concatenate([scale] * (width // LANES), axis=1)

    every = range(per_owner)
    clipped = [(scale * stacked_v[b * width : (b + 1) * width]).astype(jnp.bfloat16) for b in every]
    turned = [dot(basis_l_t[b], clipped[b]).astype(jnp.bfloat16) for b in every]
    for b in every:
        clipped_v[b] = clipped[b]
    rotated = [dot(turned[b], basis_r_v[b]) for b in every]
    normalized = []
    for b in every:
        m = BETA * first_v[b].astype(jnp.float32) + (1.0 - BETA) * rotated[b]
        v = BETA * second_v[b].astype(jnp.float32) + (1.0 - BETA) * rotated[b] * rotated[b]
        first_out[b] = m.astype(jnp.bfloat16)
        second_out[b] = v.astype(jnp.bfloat16)
        normalized.append((m / (jnp.sqrt(v) + EPS)).astype(jnp.bfloat16))
    back = [dot(basis_l_v[b], normalized[b]).astype(jnp.bfloat16) for b in every]
    updates = [dot(back[b], basis_r_v[b], ((1,), (1,))).astype(jnp.bfloat16) for b in every]
    update = jnp.concatenate(updates, axis=0)
    send_b[...] = dot(from_state[...], update).reshape(n, PIECE, width).astype(jnp.bfloat16)
    to_peers(send_b, recv_b, 5)
    recv_b[me] = send_b[me]

    def covariances(b, carry):
        block = clipped_v[b]
        cov_l_out[b] = BETA * cov_l_v[b] + (1.0 - BETA) * dot(block, block, ((1,), (1,)))
        cov_r_out[b] = BETA * cov_r_v[b] + (1.0 - BETA) * dot(block, block, ((0,), (0,)))
        return carry

    lax.fori_loop(0, per_owner, covariances, 0)

    wait_for(meta_out, n - 1, send_sem.at[1])
    wait_for(send_a, n - 1, send_sem.at[2])

    @pl.when(mine == 0)
    def _():
        wait_for(sum_in, n - 1, send_sem.at[3])
        wait_for(part_in, groups - 1, send_sem.at[4])

    @pl.when(mine != 0)
    def _():
        pltpu.make_async_copy(part_out, part_out, send_sem.at[0]).wait()

    wait_for(send_b, n - 1, send_sem.at[5])
    wait_for(recv_b, n - 1, recv_sem.at[5])
    returned = recv_b[...].astype(jnp.float32).reshape(rows, width).astype(jnp.bfloat16)
    flat_out[...] = dot(from_owner[...], returned).astype(jnp.bfloat16)


def keep(*refs):
    half = (len(refs) - 1) // 2
    sources, targets, sem = refs[:half], refs[half : 2 * half], refs[-1]
    stores = [
        pltpu.make_async_copy(source, target.at[0], sem.at[i])
        for i, (source, target) in enumerate(zip(sources, targets))
    ]
    for store in stores:
        store.start()
    for store in stores:
        store.wait()


def solution(mesh):
    n = mesh.shape["fsdp"]
    groups = mesh.shape["grp"]
    sizes = (4, n // 8, 2)

    def shard(grad, row_block, row_index, home, cov_l, cov_r, basis_l, basis_r, first, second):
        rows, width = grad.shape[1:]
        per_owner = cov_l.shape[1]
        block = (per_owner, width, width)
        f32, bf16, i32 = jnp.float32, jnp.bfloat16, jnp.int32
        vmem = pltpu.VMEM
        anywhere = pl.BlockSpec(memory_space=pl.ANY)
        here = pl.BlockSpec(memory_space=pltpu.VMEM)
        entries = float(n * groups * rows * width)
        results = pl.pallas_call(
            functools.partial(kernel, entries, sizes, groups),
            out_shape=(
                jax.ShapeDtypeStruct(block, f32),
                jax.ShapeDtypeStruct(block, f32),
                jax.ShapeDtypeStruct(block, bf16),
                jax.ShapeDtypeStruct(block, bf16),
                jax.ShapeDtypeStruct((rows, width), bf16),
            ),
            in_specs=[pl.BlockSpec(memory_space=pltpu.HBM)] * 10,
            out_specs=(here,) * 5,
            scratch_shapes=[
                vmem((rows, width), bf16),
                vmem(row_block.shape, i32),
                vmem(row_index.shape, i32),
                vmem(home.shape, i32),
                vmem(block, f32),
                vmem(block, f32),
                vmem(block, bf16),
                vmem(block, bf16),
                vmem(block, bf16),
                vmem(block, bf16),
                vmem(block, bf16),
                vmem((rows, width), f32),
                vmem(block, bf16),
                vmem((n, PIECE, width), bf16),
                vmem((n, PIECE, width), bf16),
                vmem((n, PIECE, width), bf16),
                vmem((n, PIECE, width), bf16),
                vmem((n, 1, LANES), f32),
                vmem((n, 1, LANES), f32),
                vmem((1, LANES), f32),
                vmem((groups, 1, LANES), f32),
                vmem((1, LANES), f32),
                vmem((n, 1, LANES), f32),
                vmem((1, LANES), f32),
                vmem((1, LANES), f32),
                vmem((rows, rows), bf16),
                vmem((rows, rows), bf16),
                vmem((rows, rows), bf16),
                vmem((rows, rows), bf16),
                pltpu.SemaphoreType.DMA((10,)),
                pltpu.SemaphoreType.DMA((6,)),
                pltpu.SemaphoreType.DMA((6,)),
                pltpu.SemaphoreType.REGULAR,
                pltpu.SemaphoreType.REGULAR,
            ],
            compiler_params=pltpu.CompilerParams(
                collective_id=0, has_side_effects=True, vmem_limit_bytes=24 * 1024 * 1024
            ),
            name="soap_step",
        )(
            *(
                pltpu.with_memory_space_constraint(x, pltpu.HBM)
                for x in (grad, row_block, row_index, home, cov_l, cov_r, basis_l, basis_r, first, second)
            )
        )
        return pl.pallas_call(
            keep,
            out_shape=tuple(jax.ShapeDtypeStruct((1,) + r.shape, r.dtype) for r in results),
            in_specs=[here] * 5,
            out_specs=(anywhere,) * 5,
            scratch_shapes=[pltpu.SemaphoreType.DMA((5,))],
            compiler_params=pltpu.CompilerParams(vmem_limit_bytes=8 * 1024 * 1024),
            name="keep",
        )(*results)

    flat = P("grp", "fsdp", None)
    index = P("grp", "fsdp")
    state = P("grp", "fsdp", None, None)
    return jax.shard_map(
        shard,
        mesh=mesh,
        in_specs=(flat, index, index, P("grp", None)) + (state,) * 6,
        out_specs=(state,) * 4 + (flat,),
        check_vma=False,
    )
```

```python
import functools

import jax
import jax.numpy as jnp
from jax import lax
from jax.experimental import pallas as pl
from jax.experimental.pallas import tpu as pltpu
from jax.sharding import PartitionSpec as P

MESH = pl.DeviceIdType.MESH

CLIP_RMS = 0.25
BETA = 0.95
EPS = 1e-08
PIECE = 8
LANES = 128


def iota(shape, dim):
    return lax.broadcasted_iota(jnp.int32, shape, dim)


def hot(hits):
    return jnp.where(hits, 1.0, 0.0).astype(jnp.bfloat16)


def dot(a, b, dims=((1,), (0,))):
    return lax.dot_general(a, b, (dims, ((), ())), preferred_element_type=jnp.float32)


def chip_steps(nx, ny):
    far_y = sorted(range(ny), key=lambda d: -min(d, ny - d))
    far_x = sorted(range(nx), key=lambda d: -min(d, nx - d))
    return [(dx, dy) for dy in far_y for dx in far_x if dx or dy]


def kernel(
    entries,
    sizes,
    groups,
    grad_hbm,
    row_block_hbm,
    row_index_hbm,
    home_hbm,
    cov_l_hbm,
    cov_r_hbm,
    basis_l_hbm,
    basis_r_hbm,
    first_hbm,
    second_hbm,
    cov_l_out,
    cov_r_out,
    first_out,
    second_out,
    flat_out,
    grad_v,
    row_block_v,
    row_index_v,
    home_v,
    cov_l_v,
    cov_r_v,
    basis_l_v,
    basis_r_v,
    basis_l_t,
    first_v,
    second_v,
    stacked_v,
    clipped_v,
    send_a,
    recv_a,
    send_b,
    recv_b,
    meta_out,
    meta_in,
    part_out,
    part_in,
    sum_out,
    sum_in,
    all_out,
    all_in,
    to_owner,
    from_owner,
    to_state,
    from_state,
    grad_sem,
    in_sem,
    send_sem,
    recv_sem,
    up_sem,
    down_sem,
):
    me = lax.axis_index("fsdp")
    mine = lax.axis_index("grp")
    nx, ny, nc = sizes
    n = nx * ny * nc
    rows, width = grad_v.shape
    blocks = home_v.shape[1]
    per_owner = cov_l_v.shape[0]
    per_block = width // PIECE
    my_x, my_y, my_c = me // (ny * nc), lax.rem(me // nc, ny), lax.rem(me, nc)

    def peer(dx, dy, core):
        return (lax.rem(my_x + dx, nx) * ny + lax.rem(my_y + dy, ny)) * nc + core

    partner = peer(0, 0, 1 - my_c)
    far = chip_steps(nx, ny)
    peers = [peer(dx, dy, core) for core in (1, 0) for dx, dy in far] + [partner]
    adder = peer(0, 0, 1)

    loads = [
        pltpu.make_async_copy(source, target, in_sem.at[i])
        for i, (source, target) in enumerate(
            [
                (row_block_hbm, row_block_v),
                (home_hbm, home_v),
                (row_index_hbm, row_index_v),
                (basis_l_hbm.at[0], basis_l_v),
                (basis_r_hbm.at[0], basis_r_v),
                (first_hbm.at[0], first_v),
                (second_hbm.at[0], second_v),
                (cov_l_hbm.at[0], cov_l_v),
                (cov_r_hbm.at[0], cov_r_v),
            ]
        )
    ]
    split = 4
    cut = [pl.ds(i * (rows // split), rows // split) for i in range(split)]
    grad_loads = [
        pltpu.make_async_copy(grad_hbm.at[0, part], grad_v.at[part], grad_sem.at[i])
        for i, part in enumerate(cut)
    ]
    for load in grad_loads + loads[:3]:
        load.start()

    barrier = pltpu.get_barrier_semaphore()
    row = [partner] + [peer(dx, 0, core) for dx in range(1, nx) for core in range(nc)]
    above, below = peer(0, 1, my_c), peer(0, ny - 1, my_c)
    for to in [above, below] + row:
        pl.semaphore_signal(barrier, inc=1, device_id=(to, mine), device_id_type=MESH)

    first_group = mine == 0
    adds = jnp.logical_and(first_group, my_c == 1)

    @pl.when(adds)
    def _():
        def greet(g, carry):
            pl.semaphore_signal(barrier, inc=1, device_id=(me, g), device_id_type=MESH)
            pl.semaphore_signal(barrier, inc=1, device_id=(partner, g), device_id_type=MESH)
            return carry

        lax.fori_loop(1, groups, greet, 0)

    def send(source, target, k, to):
        pltpu.make_async_remote_copy(
            source, target, send_sem.at[k], recv_sem.at[k], device_id=to, device_id_type=MESH
        ).start()

    def to_peers(source, target, k):
        for to in peers:
            send(source.at[to], target.at[me], k, (to, mine))

    def wait_for(buffer, count, sem):
        part = buffer.at[pl.ds(0, count)]
        pltpu.make_async_copy(part, part, sem).wait()

    squares = jnp.zeros((1, width), jnp.float32)
    for load, part in zip(grad_loads, cut):
        load.wait()
        wide = grad_v[part].astype(jnp.float32)
        squares += jnp.sum(wide * wide, axis=0, keepdims=True)
    total = jnp.sum(squares, axis=1, keepdims=True)
    part_out[...] = jnp.broadcast_to(total, (1, LANES))

    slot = mine * nc + my_c

    @pl.when(first_group)
    def _():
        pl.semaphore_wait(barrier, len(row) + 2)

    @pl.when(jnp.logical_not(first_group))
    def _():
        pl.semaphore_wait(barrier, len(row) + 3)

    @pl.when(adds)
    def _():
        part_in[slot] = part_out[...]

    @pl.when(jnp.logical_not(adds))
    def _():
        send(part_out, part_in.at[slot], 0, (adder, 0))

    def pass_up():
        pl.semaphore_signal(up_sem, inc=1, device_id=(above, mine), device_id_type=MESH)

    def pass_down():
        pl.semaphore_signal(down_sem, inc=1, device_id=(below, mine), device_id_type=MESH)

    pass_up()
    pass_down()

    for load in loads[3:]:
        load.start()
    for load in loads[:3]:
        load.wait()
    lookup = hot(iota((blocks, rows), 0) == row_block_v[...])
    homes = jnp.broadcast_to(home_v[...].astype(jnp.float32), (8, blocks)).astype(jnp.bfloat16)
    home = dot(homes, lookup)[0:1].astype(jnp.int32)
    owner = home // per_owner
    piece = (home % per_owner) * per_block + row_index_v[...] // PIECE
    inner = iota((1, rows), 1) % PIECE
    label = jnp.sum(
        jnp.where(iota((n, rows), 0) == owner, piece.astype(jnp.float32), 0.0), axis=1, keepdims=True
    ) * (1.0 / PIECE)
    meta_out[:, 0, :] = jnp.broadcast_to(label, (n, LANES))
    to_owner[...] = hot(iota((rows, rows), 0) == owner * PIECE + inner)
    send_a[...] = dot(to_owner[...], grad_v[...]).reshape(n, PIECE, width).astype(jnp.bfloat16)

    ups, downs = ny // 2, ny - 1 - ny // 2
    for k in range(1, ups + 1):
        pl.semaphore_wait(up_sem, 1)
        if k < ups:
            pass_up()
        if k <= downs:
            pl.semaphore_wait(down_sem, 1)
            if k < downs:
                pass_down()

    to_peers(meta_out, meta_in, 1)
    to_peers(send_a, recv_a, 2)
    meta_in[me] = meta_out[me]
    recv_a[me] = send_a[me]

    spread = dot(
        jnp.broadcast_to(owner.astype(jnp.float32), (8, rows)).astype(jnp.bfloat16),
        jnp.ones((8, LANES), jnp.bfloat16),
        ((0,), (0,)),
    )
    place = spread.astype(jnp.int32) + iota((rows, LANES), 0) % PIECE
    for c in range(rows // LANES):
        from_owner[:, c * LANES : (c + 1) * LANES] = hot(iota((rows, LANES), 1) + c * LANES == place)
    for load in loads[3:]:
        load.wait()
    for b in range(per_owner):
        basis_l_t[b] = basis_l_v[b].T

    wait_for(meta_in, n - 1, recv_sem.at[1])
    came_column = jnp.broadcast_to(meta_in[...], (n, PIECE, LANES)).reshape(rows, LANES)
    place = came_column.astype(jnp.int32) * PIECE + iota((rows, LANES), 0) % PIECE
    for c in range(rows // LANES):
        from_state[:, c * LANES : (c + 1) * LANES] = hot(iota((rows, LANES), 1) + c * LANES == place)
    came_row = dot(
        meta_in[:, 0, :].astype(jnp.bfloat16),
        hot(iota((n, rows), 0) == iota((n, rows), 1) // PIECE),
        ((0,), (0,)),
    )[0:1].astype(jnp.int32)
    to_state[...] = hot(iota((rows, rows), 0) == came_row * PIECE + inner)

    @pl.when(adds)
    def _():
        wait_for(part_in, groups * nc - 1, recv_sem.at[0])
        sum_out[...] = jnp.sum(part_in[:, 0, :], axis=0, keepdims=True)
        for to in [peer(dx, dy, core) for dx, dy in far for core in range(nc)] + [partner]:
            send(sum_out, sum_in.at[me // nc], 3, (to, mine))
        sum_in[me // nc] = sum_out[...]

    wait_for(recv_a, n - 1, recv_sem.at[2])
    arrived = recv_a[...].astype(jnp.float32).reshape(rows, width).astype(jnp.bfloat16)
    stacked_v[...] = dot(to_state[...], arrived)

    @pl.when(adds)
    def _():
        wait_for(sum_in, n // nc - 1, recv_sem.at[3])

    @pl.when(jnp.logical_and(first_group, my_c != 1))
    def _():
        wait_for(sum_in, n // nc, recv_sem.at[3])

    @pl.when(first_group)
    def _():
        all_out[...] = jnp.sum(sum_in[:, 0, :], axis=0, keepdims=True)
        all_in[...] = all_out[...]

    @pl.when(adds)
    def _():
        def tell(g, carry):
            send(all_out, all_in, 4, (partner, g))
            send(all_out, all_in, 4, (me, g))
            return carry

        lax.fori_loop(1, groups, tell, 0)

    @pl.when(jnp.logical_not(first_group))
    def _():
        pltpu.make_async_copy(all_in, all_in, recv_sem.at[4]).wait()

    scale = jnp.minimum(1.0, CLIP_RMS / jnp.sqrt(all_in[...] / entries + 1e-06))
    scale = jnp.concatenate([scale] * (width // LANES), axis=1)

    every = range(per_owner)
    clipped = [(scale * stacked_v[b * width : (b + 1) * width]).astype(jnp.bfloat16) for b in every]
    turned = [dot(basis_l_t[b], clipped[b]).astype(jnp.bfloat16) for b in every]
    for b in every:
        clipped_v[b] = clipped[b]
    rotated = [dot(turned[b], basis_r_v[b]) for b in every]
    normalized = []
    for b in every:
        m = BETA * first_v[b].astype(jnp.float32) + (1.0 - BETA) * rotated[b]
        v = BETA * second_v[b].astype(jnp.float32) + (1.0 - BETA) * rotated[b] * rotated[b]
        first_out[b] = m.astype(jnp.bfloat16)
        second_out[b] = v.astype(jnp.bfloat16)
        normalized.append((m / (jnp.sqrt(v) + EPS)).astype(jnp.bfloat16))
    back = [dot(basis_l_v[b], normalized[b]).astype(jnp.bfloat16) for b in every]
    updates = [dot(back[b], basis_r_v[b], ((1,), (1,))).astype(jnp.bfloat16) for b in every]
    update = jnp.concatenate(updates, axis=0)
    send_b[...] = dot(from_state[...], update).reshape(n, PIECE, width).astype(jnp.bfloat16)
    to_peers(send_b, recv_b, 5)
    recv_b[me] = send_b[me]

    def covariances(b, carry):
        block = clipped_v[b]
        cov_l_out[b] = BETA * cov_l_v[b] + (1.0 - BETA) * dot(block, block, ((1,), (1,)))
        cov_r_out[b] = BETA * cov_r_v[b] + (1.0 - BETA) * dot(block, block, ((0,), (0,)))
        return carry

    lax.fori_loop(0, per_owner, covariances, 0)

    wait_for(meta_out, n - 1, send_sem.at[1])
    wait_for(send_a, n - 1, send_sem.at[2])

    @pl.when(adds)
    def _():
        wait_for(meta_in, n - 1, send_sem.at[3])
        wait_for(part_in, (groups - 1) * nc, send_sem.at[4])

    @pl.when(jnp.logical_not(adds))
    def _():
        pltpu.make_async_copy(part_out, part_out, send_sem.at[0]).wait()

    wait_for(send_b, n - 1, send_sem.at[5])
    wait_for(recv_b, n - 1, recv_sem.at[5])
    returned = recv_b[...].astype(jnp.float32).reshape(rows, width).astype(jnp.bfloat16)
    flat_out[...] = dot(from_owner[...], returned).astype(jnp.bfloat16)


def keep(*refs):
    half = (len(refs) - 1) // 2
    sources, targets, sem = refs[:half], refs[half : 2 * half], refs[-1]
    stores = [
        pltpu.make_async_copy(source, target.at[0], sem.at[i])
        for i, (source, target) in enumerate(zip(sources, targets))
    ]
    for store in stores:
        store.start()
    for store in stores:
        store.wait()


def solution(mesh):
    n = mesh.shape["fsdp"]
    groups = mesh.shape["grp"]
    sizes = (4, n // 8, 2)

    def shard(grad, row_block, row_index, home, cov_l, cov_r, basis_l, basis_r, first, second):
        rows, width = grad.shape[1:]
        per_owner = cov_l.shape[1]
        block = (per_owner, width, width)
        f32, bf16, i32 = jnp.float32, jnp.bfloat16, jnp.int32
        vmem = pltpu.VMEM
        anywhere = pl.BlockSpec(memory_space=pl.ANY)
        here = pl.BlockSpec(memory_space=pltpu.VMEM)
        entries = float(n * groups * rows * width)
        results = pl.pallas_call(
            functools.partial(kernel, entries, sizes, groups),
            out_shape=(
                jax.ShapeDtypeStruct(block, f32),
                jax.ShapeDtypeStruct(block, f32),
                jax.ShapeDtypeStruct(block, bf16),
                jax.ShapeDtypeStruct(block, bf16),
                jax.ShapeDtypeStruct((rows, width), bf16),
            ),
            in_specs=[pl.BlockSpec(memory_space=pltpu.HBM)] * 10,
            out_specs=(here,) * 5,
            scratch_shapes=[
                vmem((rows, width), bf16),
                vmem(row_block.shape, i32),
                vmem(row_index.shape, i32),
                vmem(home.shape, i32),
                vmem(block, f32),
                vmem(block, f32),
                vmem(block, bf16),
                vmem(block, bf16),
                vmem(block, bf16),
                vmem(block, bf16),
                vmem(block, bf16),
                vmem((rows, width), f32),
                vmem(block, bf16),
                vmem((n, PIECE, width), bf16),
                vmem((n, PIECE, width), bf16),
                vmem((n, PIECE, width), bf16),
                vmem((n, PIECE, width), bf16),
                vmem((n, 1, LANES), f32),
                vmem((n, 1, LANES), f32),
                vmem((1, LANES), f32),
                vmem((groups * sizes[2], 1, LANES), f32),
                vmem((1, LANES), f32),
                vmem((n // sizes[2], 1, LANES), f32),
                vmem((1, LANES), f32),
                vmem((1, LANES), f32),
                vmem((rows, rows), bf16),
                vmem((rows, rows), bf16),
                vmem((rows, rows), bf16),
                vmem((rows, rows), bf16),
                pltpu.SemaphoreType.DMA((4,)),
                pltpu.SemaphoreType.DMA((9,)),
                pltpu.SemaphoreType.DMA((6,)),
                pltpu.SemaphoreType.DMA((6,)),
                pltpu.SemaphoreType.REGULAR,
                pltpu.SemaphoreType.REGULAR,
            ],
            compiler_params=pltpu.CompilerParams(
                collective_id=0, has_side_effects=True, vmem_limit_bytes=24 * 1024 * 1024
            ),
            name="soap_step",
        )(
            *(
                pltpu.with_memory_space_constraint(x, pltpu.HBM)
                for x in (grad, row_block, row_index, home, cov_l, cov_r, basis_l, basis_r, first, second)
            )
        )
        return pl.pallas_call(
            keep,
            out_shape=tuple(jax.ShapeDtypeStruct((1,) + r.shape, r.dtype) for r in results),
            in_specs=[here] * 5,
            out_specs=(anywhere,) * 5,
            scratch_shapes=[pltpu.SemaphoreType.DMA((5,))],
            compiler_params=pltpu.CompilerParams(vmem_limit_bytes=8 * 1024 * 1024),
            name="keep",
        )(*results)

    flat = P("grp", "fsdp", None)
    index = P("grp", "fsdp")
    state = P("grp", "fsdp", None, None)
    return jax.shard_map(
        shard,
        mesh=mesh,
        in_specs=(flat, index, index, P("grp", None)) + (state,) * 6,
        out_specs=(state,) * 4 + (flat,),
        check_vma=False,
    )
```
